128 devices in a mesh: dp: 2 (over core), ep: 64 (over x, y, z).
Axes of the slice: x: 4, y: 4, z: 4, core: 2. Of those that a mesh axis runs over, the one named last changes fastest.
Arguments:
- x: bfloat16 [2, 64, 256, 2048], P('dp', 'ep'), parts along dimension 0
- expert: int32 [2, 64, 256, 8], P('dp', 'ep'), parts along dimension 0
- slot: int32 [2, 64, 256, 8], P('dp', 'ep'), parts along dimension 0
- gate: float32 [2, 64, 256, 8], P('dp', 'ep'), parts along dimension 0
- w_gate: bfloat16 [128, 2048, 1408], P('ep')
- w_up: bfloat16 [128, 2048, 1408], P('ep')
- w_down: bfloat16 [128, 1408, 2048], P('ep')
- s_gate: bfloat16 [2048, 1408], replicated
- s_up: bfloat16 [2048, 1408], replicated
- s_down: bfloat16 [1408, 2048], replicated
Outputs:
- y: bfloat16 [2, 64, 256, 2048], P('dp', 'ep'), parts along dimension 0
There are 2 independent parts. The reference program is written for one: setup_inputs(seed, part) draws one part's arguments, and reference() takes and returns one part's arrays. A program takes and returns all parts, laid end to end along the dimension named above; an argument that names none is the same for every part.
All inputs are finite; a program needn't handle non-finite values.
Results may differ from the reference program's by a relative error of at most 0.009.
Values are sent between devices in bfloat16 or wider.
A program may use at most 1.5 GiB of HBM per device.

```python
import jax
import jax.numpy as jnp

MEMBERS = 64
TOKENS = 256
D = 2048
FF = 1408
TOP = 8
EXPERTS = 128
SHARED_FF = 1408
SLOTS = 5 * TOKENS * TOP // (4 * EXPERTS)


def setup_inputs(seed: int = 0, part: int = 0) -> dict:
    own, k1, k2, k3, k4, k5, k6 = jax.random.split(jax.random.key(seed), 7)
    kx, ke, kl, kg = jax.random.split(jax.random.fold_in(own, part), 4)
    devices = (1, MEMBERS)
    place = jax.random.permutation(kl, jnp.arange(EXPERTS, dtype=jnp.uint32))
    slow = ((EXPERTS + (9 * place) % EXPERTS) << ((9 * place) // EXPERTS)) // EXPERTS
    wait = (jax.random.bits(ke, (*devices, TOKENS, EXPERTS), jnp.uint32) >> 10) * slow
    expert = jnp.argsort(wait, axis=-1)[..., :TOP].astype(jnp.int32)
    chosen = jax.nn.one_hot(expert, EXPERTS, dtype=jnp.int32)
    in_line = jnp.cumsum(chosen.reshape(*devices, TOKENS * TOP, EXPERTS), axis=2) - 1
    slot = jnp.sum(in_line.reshape(chosen.shape) * chosen, axis=-1)

    def one(key, rows, columns):
        return (jax.random.normal(key, (rows, columns), jnp.float32) * rows**-0.5).astype(jnp.bfloat16)

    def weights(key, rows, columns):
        return jax.lax.map(lambda k: one(k, rows, columns), jax.random.split(key, EXPERTS))

    return {
        "x": jax.random.normal(kx, (*devices, TOKENS, D), jnp.float32).astype(jnp.bfloat16),
        "expert": expert,
        "slot": slot,
        "gate": jax.nn.softmax(jax.random.normal(kg, expert.shape, jnp.float32)),
        "w_gate": weights(k1, D, FF),
        "w_up": weights(k2, D, FF),
        "w_down": weights(k3, FF, D),
        "s_gate": one(k4, D, SHARED_FF),
        "s_up": one(k5, D, SHARED_FF),
        "s_down": one(k6, SHARED_FF, D),
    }


def einsum(form, a, b):
    return jnp.einsum(form, a.astype(jnp.float32), b.astype(jnp.float32))


def for_all(x, s_gate, s_up, s_down):
    h = jax.nn.silu(einsum("...d,df->...f", x, s_gate)) * einsum("...d,df->...f", x, s_up)
    return einsum("...f,fd->...d", h.astype(jnp.bfloat16), s_down)


def reference(x, expert, slot, gate, w_gate, w_up, w_down, s_gate, s_up, s_down):
    to_expert = jax.nn.one_hot(expert, EXPERTS, dtype=jnp.bfloat16)
    to_slot = jax.nn.one_hot(slot, SLOTS, dtype=jnp.bfloat16)
    weighted = to_expert * gate[..., None].astype(jnp.bfloat16)
    dispatch = einsum("abtke,abtkc->abtec", to_expert, to_slot).astype(jnp.bfloat16)
    combine = einsum("abtke,abtkc->abtec", weighted, to_slot).astype(jnp.bfloat16)
    z = einsum("abtec,abtd->aebcd", dispatch, x).astype(jnp.bfloat16)
    h = jax.nn.silu(einsum("aebcd,edf->aebcf", z, w_gate))
    h = (h * einsum("aebcd,edf->aebcf", z, w_up)).astype(jnp.bfloat16)
    out = einsum("aebcf,efd->aebcd", h, w_down).astype(jnp.bfloat16)
    y = einsum("abtec,aebcd->abtd", combine, out)
    return (y + for_all(x, s_gate, s_up, s_down)).astype(jnp.bfloat16)
```

```python
import jax
import jax.numpy as jnp
from jax import lax
from jax.sharding import PartitionSpec as P

BF, F32 = jnp.bfloat16, jnp.float32


def dot(a, b, dims=(((1,), (0,)), ((), ()))):
    return lax.dot_general(a, b, dims, preferred_element_type=F32)


def mlp(z, g, u, d):
    h = jax.nn.silu(dot(z, g)) * dot(z, u)
    return dot(h.astype(BF), d)


def solution(mesh):
    members = mesh.shape["ep"]

    def body(x, expert, slot, gate, w_gate, w_up, w_down, s_gate, s_up, s_down):
        x, expert, slot, gate = x[0, 0], expert[0, 0], slot[0, 0], gate[0, 0]
        (tokens, width), top = x.shape, expert.shape[1]
        here = w_gate.shape[0]
        experts = here * members
        slots = 5 * tokens * top // (4 * experts)
        rows = here * slots
        e, s = expert.reshape(-1), slot.reshape(-1)
        in_expert = jax.nn.one_hot(e, experts, dtype=BF)
        in_slot = jax.nn.one_hot(s, slots, dtype=BF)
        number = (jnp.arange(tokens * top, dtype=jnp.int32) // top + 1).astype(BF)
        weight = gate.reshape(-1).astype(BF)
        both = jnp.concatenate([in_slot * number[:, None], in_slot * weight[:, None]], axis=1)
        table = dot(in_expert, both, (((0,), (0,)), ((), ())))
        token = table[:, :slots].reshape(-1).astype(jnp.int32) - 1
        weight = table[:, slots:].reshape(-1)
        hit = token[:, None] == jnp.arange(tokens, dtype=jnp.int32)[None]
        z = dot(hit.astype(BF), x).astype(BF)
        z = lax.all_to_all(z.reshape(members, rows, width), "ep", 0, 0, tiled=True)
        z = z.reshape(members, here, slots, width)
        outs = []
        for i in range(here):
            zi = z[:, i].reshape(members * slots, width)
            outs.append(mlp(zi, w_gate[i], w_up[i], w_down[i]).astype(BF).reshape(members, slots, width))
        out = jnp.concatenate(outs, axis=1)
        out = lax.all_to_all(out, "ep", 0, 0, tiled=True).reshape(members * rows, width)
        combine = jnp.where(hit, weight[:, None], 0.0).astype(BF)
        y = dot(combine, out, (((0,), (0,)), ((), ())))
        y = y + mlp(x, s_gate, s_up, s_down)
        return y.astype(BF)[None, None]

    one, all_ = P("dp", "ep"), P()
    return jax.shard_map(
        body,
        mesh=mesh,
        in_specs=(one, one, one, one, P("ep"), P("ep"), P("ep"), all_, all_, all_),
        out_specs=one,
        check_vma=False,
    )
```
